32 devices in a mesh: ta: 4 (over y, x), gz: 4 (over z), xy: 2 (over core).
Axes of the slice: x: 2, y: 2, z: 4, core: 2. Of those that a mesh axis runs over, the one named last changes fastest.
Arguments:
- links: float32 [4, 2, 3, 3, 8, 8, 256], P(None, None, None, None, 'ta', 'gz', 'xy'), may hold values from -1 to 1, as said below
- solutions: float32 [2, 2, 4, 3, 8, 8, 256], P(None, None, None, None, 'ta', 'gz', 'xy'), may hold values from -6 to 6
Outputs:
- force: float32 [4, 2, 3, 3, 8, 8, 256], P(None, None, None, None, 'ta', 'gz', 'xy')
The draws below stay inside these ranges and needn't reach their ends.
Inputs may be any that keep to these rules, and one draw needn't show every extreme that they name: Each links[mu] at a site, read as a complex 3 x 3 matrix, is special unitary.
All inputs are finite; a program needn't handle non-finite values.
Results may differ from the reference program's by a relative error of at most 0.0001.
Values sent between devices are 32-bit elements; how exact they have to be, the bound alone decides.
A program may use at most 64 MiB of HBM per device.

```python
import math
from functools import reduce
import jax
import jax.numpy as jnp
import numpy as np
from jax import lax

Y_LEN = 64
NSOL = 2
NT = 8
NZ = 8
NXY = 256


def embed_rotation(turning, phase_one, phase_two, first, second):
    zeros = jnp.zeros_like(turning)
    ones = jnp.ones_like(turning)
    real_rows = [[ones if row == column else zeros for column in range(3)] for row in range(3)]
    imaginary_rows = [[zeros for column in range(3)] for row in range(3)]
    cosine = jnp.cos(turning)
    sine = jnp.sin(turning)
    alpha_real = cosine * jnp.cos(phase_one)
    alpha_imaginary = cosine * jnp.sin(phase_one)
    beta_real = sine * jnp.cos(phase_two)
    beta_imaginary = sine * jnp.sin(phase_two)
    real_rows[first][first] = alpha_real
    imaginary_rows[first][first] = alpha_imaginary
    real_rows[first][second] = beta_real
    imaginary_rows[first][second] = beta_imaginary
    real_rows[second][first] = -beta_real
    imaginary_rows[second][first] = beta_imaginary
    real_rows[second][second] = alpha_real
    imaginary_rows[second][second] = -alpha_imaginary
    real_matrix = jnp.stack([jnp.stack(row, 0) for row in real_rows], 0)
    imaginary_matrix = jnp.stack([jnp.stack(row, 0) for row in imaginary_rows], 0)
    return (real_matrix, imaginary_matrix)


def complex_matmul(left, right):
    real_part = jnp.einsum('ab...,bc...->ac...', left[0], right[0]) - jnp.einsum('ab...,bc...->ac...', left[1], right[1])
    imaginary_part = jnp.einsum('ab...,bc...->ac...', left[0], right[1]) + jnp.einsum('ab...,bc...->ac...', left[1], right[0])
    return (real_part, imaginary_part)


def draw_links(key, part):
    subkeys = jax.random.split(key, 9)
    draw_shape = (4, NT, NZ, NXY)
    angles = [jax.random.uniform(subkeys[index], draw_shape, jnp.float32, 0.0, 2.0 * math.pi) for index in range(9)]
    planes = ((0, 1), (1, 2), (0, 2))
    product = None
    for plane_index in range(3):
        rotation = embed_rotation(angles[3 * plane_index], angles[3 * plane_index + 1], angles[3 * plane_index + 2], planes[plane_index][0], planes[plane_index][1])
        product = rotation if product is None else complex_matmul(product, rotation)
    stacked = jnp.stack([product[0], product[1]], 0)
    return jnp.moveaxis(stacked, 3, 0).astype(jnp.float32)


def block_levels(rng, dims, shards, smallest, high):
    def one(position, shards_of):
        draws = jax.random.uniform(jax.random.fold_in(jax.random.fold_in(rng, 6), position), (shards_of,), jnp.float32, smallest / len(shards), high / len(shards))
        return jnp.repeat(jnp.exp(draws), dims[position] // shards_of).reshape((-1,) + (1,) * (len(dims) - position - 1))

    gain = one(*shards[0])
    for cut in shards[1:]:
        gain = gain * one(*cut)
    return gain


def centred(own_key, dims, spread, limit, cuts=(), kind=jnp.bfloat16):
    values = jax.random.normal(own_key, dims, jnp.float32) * spread
    if len(cuts) > 0:
        values = block_levels(own_key, dims, cuts, -0.22, 0.18) * values
    return jnp.clip(values, min=-limit, max=limit).astype(kind)


def setup_inputs(seed: int = 0) -> dict:
    streams_of = jax.random.split(jax.random.key(seed), 3)
    links = draw_links(jax.random.fold_in(streams_of[2], 71), 0)
    solutions = centred(streams_of[1], (NSOL, 2, 4, 3, NT, NZ, NXY), 1.0, 6.0, ((4, 4), (5, 4), (6, 2)), jnp.float32)
    return dict(links=links, solutions=solutions)


HOPPING = 0.125
PLAQUETTE = 0.5


def projectors():
    identity = np.eye(4)
    zeros = np.zeros((4, 4))
    gamma_time = (np.array([[0, 0, 1, 0], [0, 0, 0, 1], [1, 0, 0, 0], [0, 1, 0, 0]]), zeros)
    gamma_depth = (zeros, np.array([[0, 0, 1, 0], [0, 0, 0, -1], [-1, 0, 0, 0], [0, 1, 0, 0]]))
    gamma_across = (zeros, np.array([[0, 0, 0, 1], [0, 0, 1, 0], [0, -1, 0, 0], [-1, 0, 0, 0]]))
    gamma_along = (np.array([[0, 0, 0, -1], [0, 0, 1, 0], [0, 1, 0, 0], [-1, 0, 0, 0]]), zeros)
    result = []
    for gamma_pair in (gamma_time, gamma_depth, gamma_across, gamma_along):
        result.append(((identity - gamma_pair[0], -gamma_pair[1]), (identity + gamma_pair[0], gamma_pair[1])))
    return result


def shift_rows(source, stride, row_length):
    positions = lax.iota(jnp.int32, source.shape[-1]) % row_length
    if stride > 0:
        return jnp.where(positions == row_length - 1, jnp.roll(source, row_length - 1, -1), jnp.roll(source, -1, -1))
    return jnp.where(positions == 0, jnp.roll(source, 1 - row_length, -1), jnp.roll(source, 1, -1))


def displace(source, direction, stride):
    if direction == 0:
        return jnp.roll(source, -stride, axis=-3)
    if direction == 1:
        return jnp.roll(source, -stride, axis=-2)
    if direction == 2:
        return jnp.roll(source, -stride * Y_LEN, axis=-1)
    return shift_rows(source, stride, Y_LEN)


def displace_spinor(source, direction, stride):
    displaced = displace(source, direction, stride)
    if direction == 0:
        positions = lax.iota(jnp.int32, NT)
        boundary = NT - 1 if stride > 0 else 0
        factor = jnp.where(positions == boundary, -1.0, 1.0).astype(source.dtype)
        displaced = displaced * factor[:, None, None]
    return displaced


def matrix_product(left, right):
    left_real, left_imaginary = left[0], left[1]
    right_real, right_imaginary = right[0], right[1]
    real_part = jnp.sum(left_real[:, :, None] * right_real[None] - left_imaginary[:, :, None] * right_imaginary[None], axis=1)
    imaginary_part = jnp.sum(left_real[:, :, None] * right_imaginary[None] + left_imaginary[:, :, None] * right_real[None], axis=1)
    return jnp.stack([real_part, imaginary_part])


def dagger(matrix):
    return jnp.stack([jnp.swapaxes(matrix[0], 0, 1), -jnp.swapaxes(matrix[1], 0, 1)])


def colour_apply(matrix, spinor):
    matrix_real = matrix[0][None, None]
    matrix_imaginary = matrix[1][None, None]
    spinor_real = spinor[:, 0][:, :, None]
    spinor_imaginary = spinor[:, 1][:, :, None]
    real_part = jnp.sum(matrix_real * spinor_real - matrix_imaginary * spinor_imaginary, axis=3)
    imaginary_part = jnp.sum(matrix_real * spinor_imaginary + matrix_imaginary * spinor_real, axis=3)
    return jnp.stack([real_part, imaginary_part], axis=1)


def spin_apply(projector, spinor):
    spinor_real = spinor[:, 0]
    spinor_imaginary = spinor[:, 1]
    rows_real = []
    rows_imaginary = []
    for spin_row in range(4):
        terms_real = []
        terms_imaginary = []
        for spin_column in range(4):
            weight_real = float(projector[0][spin_row, spin_column])
            weight_imaginary = float(projector[1][spin_row, spin_column])
            terms_real.append(weight_real * spinor_real[:, spin_column] - weight_imaginary * spinor_imaginary[:, spin_column])
            terms_imaginary.append(weight_real * spinor_imaginary[:, spin_column] + weight_imaginary * spinor_real[:, spin_column])
        rows_real.append(reduce(jnp.add, terms_real))
        rows_imaginary.append(reduce(jnp.add, terms_imaginary))
    return jnp.stack([jnp.stack(rows_real, 1), jnp.stack(rows_imaginary, 1)], 1)


def spin_outer(upper_spinor, lower_spinor):
    upper_real = upper_spinor[:, 0][:, :, :, None]
    upper_imaginary = upper_spinor[:, 1][:, :, :, None]
    lower_real = lower_spinor[:, 0][:, :, None]
    lower_imaginary = lower_spinor[:, 1][:, :, None]
    real_part = jnp.sum(upper_real * lower_real + upper_imaginary * lower_imaginary, axis=(0, 1))
    imaginary_part = jnp.sum(upper_imaginary * lower_real - upper_real * lower_imaginary, axis=(0, 1))
    return jnp.stack([real_part, imaginary_part])


def traceless_part(matrix):
    real_part = 0.5 * (matrix[0] - jnp.swapaxes(matrix[0], 0, 1))
    imaginary_part = 0.5 * (matrix[1] + jnp.swapaxes(matrix[1], 0, 1))
    trace_third = (imaginary_part[0, 0] + imaginary_part[1, 1] + imaginary_part[2, 2]) / 3.0
    identity = jnp.eye(3, dtype=matrix.dtype).reshape((3, 3) + (1,) * (matrix.ndim - 3))
    imaginary_part = imaginary_part - identity * trace_third
    return jnp.stack([real_part, imaginary_part])


def reference(links, solutions):
    projector_list = projectors()
    hop_terms = []
    for direction in range(4):
        minus_projector, plus_projector = projector_list[direction]
        forward = colour_apply(links[direction], spin_apply(minus_projector, displace_spinor(solutions, direction, 1)))
        backward = colour_apply(dagger(displace(links[direction], direction, -1)), spin_apply(plus_projector, displace_spinor(solutions, direction, -1)))
        hop_terms.append(forward + backward)
    partner = solutions - HOPPING * reduce(jnp.add, hop_terms)
    forces = []
    for direction in range(4):
        minus_projector, plus_projector = projector_list[direction]
        link_main = links[direction]
        pieces = []
        for second in range(4):
            if second == direction:
                continue
            link_second = links[second]
            upper_staple = matrix_product(matrix_product(displace(link_second, direction, 1), dagger(displace(link_main, second, 1))), dagger(link_second))
            shifted_back = displace(link_second, second, -1)
            lower_staple = matrix_product(matrix_product(dagger(displace(shifted_back, direction, 1)), dagger(displace(link_main, second, -1))), shifted_back)
            pieces.append(upper_staple + lower_staple)
        staple = reduce(jnp.add, pieces)
        fermion = spin_outer(spin_apply(minus_projector, displace_spinor(solutions, direction, 1)), partner) + spin_outer(spin_apply(plus_projector, displace_spinor(partner, direction, 1)), solutions)
        forces.append(traceless_part(matrix_product(link_main, PLAQUETTE * staple + HOPPING * fermion)))
    return jnp.stack(forces)
```

```python
import functools

import jax
import jax.numpy as jnp
from jax import lax
from jax.experimental import pallas as pl
from jax.experimental.pallas import tpu as pltpu
from jax.sharding import PartitionSpec as P

Y_LEN = 64
HOPPING = 0.125
PLAQUETTE = 0.5
AXES = ("ta", "gz", "xy")
MESH = pl.DeviceIdType.MESH

SIGMA = (
    ((0, 0), (1, 0)),
    ((0, 1), (1, 3)),
    ((1, 1), (0, 1)),
    ((1, 2), (0, 0)),
)


def phased(value, power):
    re, im = value
    return ((re, im), (-im, re), (-re, -im), (im, -re))[power % 4]


def added(a, b, sign):
    if sign > 0:
        return a[0] + b[0], a[1] + b[1]
    return a[0] - b[0], a[1] - b[1]


def half(x, mu, sign):
    rows = []
    for s in range(2):
        column, power = SIGMA[mu][s]
        lower = phased((x[0][2 + column], x[1][2 + column]), power)
        rows.append(added((x[0][s], x[1][s]), lower, sign))
    return jnp.stack([rows[0][0], rows[1][0]]), jnp.stack([rows[0][1], rows[1][1]])


def full_rows(h, mu, sign):
    lower = [None, None]
    for s in range(2):
        column, power = SIGMA[mu][s]
        lower[column] = phased((h[0][s], h[1][s]), (-power if sign > 0 else 2 - power))
    return [(h[0][0], h[1][0]), (h[0][1], h[1][1])] + lower


def product(left, right, left_dagger=False, right_dagger=False):
    re = im = None
    for k in range(3):
        ar, ai = (left[0][k], left[1][k]) if left_dagger else (left[0][:, k], left[1][:, k])
        br, bi = (right[0][:, k], right[1][:, k]) if right_dagger else (right[0][k], right[1][k])
        ar, ai, br, bi = ar[:, None], ai[:, None], br[None], bi[None]
        rr, ii, ri, ir = ar * br, ai * bi, ar * bi, ai * br
        same = left_dagger == right_dagger
        re_k = rr - ii if same else rr + ii
        if left_dagger:
            im_k = -(ri + ir) if right_dagger else ri - ir
        else:
            im_k = ir - ri if right_dagger else ri + ir
        re = re_k if re is None else re + re_k
        im = im_k if im is None else im + im_k
    return re, im


def colour(u, h, dagger=False):
    re = im = None
    for k in range(3):
        ur, ui = (u[0][k], u[1][k]) if dagger else (u[0][:, k], u[1][:, k])
        ur, ui = ur[None], ui[None]
        hr, hi = h[0][:, k][:, None], h[1][:, k][:, None]
        if dagger:
            re_k, im_k = ur * hr + ui * hi, ur * hi - ui * hr
        else:
            re_k, im_k = ur * hr - ui * hi, ur * hi + ui * hr
        re = re_k if re is None else re + re_k
        im = im_k if im is None else im + im_k
    return re, im


def outer(f, g):
    re = im = None
    for s in range(2):
        fr, fi = f[0][s][:, None], f[1][s][:, None]
        gr, gi = g[0][s][None], g[1][s][None]
        re_s, im_s = fr * gr + fi * gi, fi * gr - fr * gi
        re = re_s if re is None else re + re_s
        im = im_s if im is None else im + im_s
    return re, im


def nine(m, scale):
    re, im = m
    pairs = ((0, 1), (0, 2), (1, 2))
    parts = [(re[i, j] - re[j, i]) * (0.5 * scale) for i, j in pairs]
    parts += [(im[i, j] + im[j, i]) * (0.5 * scale) for i, j in pairs]
    parts += [im[i, i] * scale for i in range(3)]
    return jnp.stack(parts)


def roll(value, by):
    lanes = value.shape[-1]
    return pltpu.roll(value, by % lanes, value.ndim - 1)


def y_shift(value, stride):
    lanes = value.shape[-1]
    at = lax.broadcasted_iota(jnp.int32, value.shape, value.ndim - 1) % Y_LEN
    if stride > 0:
        return jnp.where(at == Y_LEN - 1, roll(value, Y_LEN - 1), roll(value, lanes - 1))
    return jnp.where(at == 0, roll(value, lanes - Y_LEN + 1), roll(value, 1))


def r_ahead(here, ahead):
    lane = lax.broadcasted_iota(jnp.int32, here.shape, here.ndim - 1)
    return roll(jnp.where(lane < Y_LEN, ahead, here), here.shape[-1] - Y_LEN)


def r_behind(here, behind):
    lanes = here.shape[-1]
    lane = lax.broadcasted_iota(jnp.int32, here.shape, here.ndim - 1)
    return roll(jnp.where(lane >= lanes - Y_LEN, behind, here), Y_LEN)


def offsets(sizes):
    t, z, r = (1, 0, 0), (0, 1, 0), (0, 0, 1)
    steps = [t, z, r]
    steps += [(1, -1, 0), (1, 0, -1), (0, 1, -1)]
    both = steps + [tuple(-c for c in step) for step in steps]
    unique = []
    for step in both:
        seat = tuple(c % n for c, n in zip(step, sizes))
        if seat not in unique:
            unique.append(seat)
    return unique


LOCAL_COPIES = 64
REMOTE_COPIES = 96


def kernel(sizes, block, links, solutions, force, *refs):
    (ul, utp, utm, uzp, uzm, urf, urb, urp, urm, uyp, uym, edges, far, xs,
     xtp, xtm, xzp, xzm, xrf, xrb, ys, hy, hyn, ws, fs, gs, local, sends, recvs) = refs
    blocks_t, blocks_z = block
    rows, lanes = ul.shape[-2:]
    solves = xs.shape[-2] // rows
    last_t, last_z = blocks_t - 1, blocks_z - 1
    one_ring = sizes[2] == 2
    if one_ring:
        urb, xrb = urf, xrf
    me = [lax.axis_index(axis) for axis in AXES]

    def seat(step):
        return {
            axis: m if c % n == 0 else lax.rem(m + (c % n), n)
            for axis, m, c, n in zip(AXES, me, step, sizes)
        }

    every_t, every_z = (0, blocks_t), (0, blocks_z)

    def runs(box_t, box_z):
        (t, many_t), (z, many_z) = box_t, box_z
        if many_z == blocks_z:
            return [(t * blocks_z, many_t * blocks_z)]
        return [((t + k) * blocks_z + z, many_z) for k in range(many_t)]

    head_t, tail_t, zero, edge_t = (0, last_t), (1, last_t), (0, 1), (last_t, 1)
    head_z, tail_z, edge_z = (0, last_z), (1, last_z), (last_z, 1)

    locals_, remotes = [], []

    def bring(source, target):
        copy = pltpu.make_async_copy(source, target, local.at[len(locals_)])
        copy.start()
        locals_.append(copy)

    def send(source, target, step):
        k = len(remotes)
        copy = pltpu.make_async_remote_copy(
            src_ref=source, dst_ref=target, send_sem=sends.at[k], recv_sem=recvs.at[k],
            device_id=seat(step), device_id_type=MESH,
        )
        copy.start()
        remotes.append(copy)

    def boxes(source, from_box, target, to_box, lead, one):
        everything = (slice(None),) * lead
        for (a, n), (b, _) in zip(runs(*from_box), runs(*to_box)):
            one(source.at[(*everything, pl.ds(a, n))], target.at[(*everything, pl.ds(b, n))])

    def spinor_boxes(source, from_box, target, to_box, lead, one):
        everything = (slice(None),) * lead
        for s in range(solves):
            for (a, n), (b, _) in zip(runs(*from_box), runs(*to_box)):
                one(
                    source.at[(*everything, pl.ds(s * rows + a, n))],
                    target.at[(*everything, pl.ds(s * rows + b, n))],
                )

    bring(links, ul)
    for n in range(solves):
        bring(solutions.at[n], xs.at[:, :, :, pl.ds(n * rows, rows)])
    first_locals = len(locals_)
    boxes(links, (tail_t, every_z), utp, (head_t, every_z), 4, bring)
    boxes(links, (head_t, every_z), utm, (tail_t, every_z), 4, bring)
    boxes(links, (every_t, tail_z), uzp, (every_t, head_z), 4, bring)
    boxes(links, (every_t, head_z), uzm, (every_t, tail_z), 4, bring)
    boxes(links.at[1], (tail_t, head_z), edges.at[0], (head_t, tail_z), 3, bring)
    boxes(links.at[0], (head_t, tail_z), edges.at[1], (tail_t, head_z), 3, bring)

    barrier = pltpu.get_barrier_semaphore()
    peers = offsets(sizes)
    for step in peers:
        pl.semaphore_signal(barrier, inc=1, device_id=seat(step), device_id_type=MESH)
    for copy in locals_[:first_locals]:
        copy.wait()
    pl.semaphore_wait(barrier, len(peers))

    t_ahead, t_behind, z_ahead, z_behind = (1, 0, 0), (-1, 0, 0), (0, 1, 0), (0, -1, 0)
    r_next, r_prev = (0, 0, 1), (0, 0, -1)

    def sent(source, from_t, from_z, target, to_t, to_z, lead, step):
        boxes(source, (from_t, from_z), target, (to_t, to_z), lead,
              lambda a, b: send(a, b, step))

    def sent_spinor(source, from_t, from_z, target, to_t, to_z, lead, step):
        spinor_boxes(source, (from_t, from_z), target, (to_t, to_z), lead,
                     lambda a, b: send(a, b, step))

    sent_spinor(xs, zero, every_z, xtp, edge_t, every_z, 3, t_behind)
    sent_spinor(xs, edge_t, every_z, xtm, zero, every_z, 3, t_ahead)
    sent_spinor(xs, every_t, zero, xzp, every_t, edge_z, 3, z_behind)
    sent_spinor(xs, every_t, edge_z, xzm, every_t, zero, 3, z_ahead)
    sent(ul.at[0], edge_t, every_z, utm.at[0], zero, every_z, 3, t_ahead)
    sent(ul.at[1], every_t, edge_z, uzm.at[1], every_t, zero, 3, z_ahead)
    send(xs, xrf, r_prev)
    if not one_ring:
        send(xs, xrb, r_next)
    send(ul.at[2], urb.at[2], r_prev if one_ring else r_next)
    first_remotes = len(remotes)
    later, other = pl.ds(1, 3), pl.ds(2, 2)
    sent(ul.at[later], zero, every_z, utp.at[later], edge_t, every_z, 4, t_behind)
    sent(ul.at[later], edge_t, every_z, utm.at[later], zero, every_z, 4, t_ahead)
    sent(ul.at[0], every_t, zero, uzp.at[0], every_t, edge_z, 3, z_behind)
    sent(ul.at[other], every_t, zero, uzp.at[other], every_t, edge_z, 4, z_behind)
    sent(ul.at[0], every_t, edge_z, uzm.at[0], every_t, zero, 3, z_ahead)
    sent(ul.at[other], every_t, edge_z, uzm.at[other], every_t, zero, 4, z_ahead)
    sent(ul.at[1], tail_t, edge_z, edges.at[0], head_t, zero, 3, z_ahead)
    sent(ul.at[1], zero, edge_z, edges.at[0], edge_t, zero, 3, (-1, 1, 0))
    sent(ul.at[1], zero, head_z, edges.at[0], edge_t, tail_z, 3, t_behind)
    sent(ul.at[0], edge_t, tail_z, edges.at[1], zero, head_z, 3, t_ahead)
    sent(ul.at[0], edge_t, zero, edges.at[1], zero, edge_z, 3, (1, -1, 0))
    sent(ul.at[0], head_t, zero, edges.at[1], tail_t, edge_z, 3, z_behind)
    sent(ul.at[2], zero, every_z, far.at[0], edge_t, every_z, 3, (-1, 0, 1))
    sent(ul.at[0], edge_t, every_z, far.at[1], zero, every_z, 3, (1, 0, -1))
    sent(ul.at[2], every_t, zero, far.at[2], every_t, edge_z, 3, (0, -1, 1))
    sent(ul.at[1], every_t, edge_z, far.at[3], every_t, zero, 3, (0, 1, -1))
    sent(ul.at[2], tail_t, every_z, far.at[0], head_t, every_z, 3, r_next)
    sent(ul.at[0], head_t, every_z, far.at[1], tail_t, every_z, 3, r_prev)
    sent(ul.at[2], every_t, tail_z, far.at[2], every_t, head_z, 3, r_next)
    sent(ul.at[1], every_t, head_z, far.at[3], every_t, tail_z, 3, r_prev)
    send(ul.at[pl.ds(0, 2)], urf.at[pl.ds(0, 2)], r_prev)
    send(ul.at[3], urf.at[3], r_prev)
    if not one_ring:
        send(ul.at[pl.ds(0, 2)], urb.at[pl.ds(0, 2)], r_next)
        send(ul.at[3], urb.at[3], r_next)
    link_remotes = len(remotes)
    spinor_boxes(xs, (tail_t, every_z), xtp, (head_t, every_z), 3, bring)
    spinor_boxes(xs, (head_t, every_z), xtm, (tail_t, every_z), 3, bring)
    spinor_boxes(xs, (every_t, tail_z), xzp, (every_t, head_z), 3, bring)
    spinor_boxes(xs, (every_t, head_z), xzm, (every_t, tail_z), 3, bring)

    def spinor(ref):
        return ref[0], ref[1]

    def gauge(ref, mu):
        return ref[mu, 0], ref[mu, 1]

    def put(ref, mu, value):
        ref[mu, 0], ref[mu, 1] = value

    def doubled(ref, mu):
        re, im = gauge(ref, mu)
        return jnp.concatenate([re] * solves, 2), jnp.concatenate([im] * solves, 2)

    def both(f, *values):
        return tuple(f(*parts) for parts in zip(*values))

    index = lax.broadcasted_iota(jnp.int32, (solves * rows, lanes), 0)
    index = (index // blocks_z) % blocks_t
    wraps_ahead = (index == last_t) & (me[0] == sizes[0] - 1)
    wraps_behind = (index == 0) & (me[0] == 0)
    ahead_sign = jnp.where(wraps_ahead, -1.0, 1.0)
    behind_sign = jnp.where(wraps_behind, -1.0, 1.0)

    def signed(h, sign):
        return both(lambda v: v * sign, h)

    def y_up(value):
        return both(lambda v: y_shift(v, 1), value)

    def y_down(value):
        return both(lambda v: y_shift(v, -1), value)

    for mu in range(4):
        here = gauge(ul, mu)
        if mu < 3:
            put(uyp, mu, y_up(here))
        put(uym, mu, y_down(here))

    for copy in locals_[first_locals:]:
        copy.wait()
    for copy in remotes[:first_remotes]:
        copy.wait_recv()

    put(urm, 2, both(r_behind, gauge(ul, 2), gauge(urb, 2)))

    x = spinor(xs)
    total = [None] * 4

    def gather(w, mu, sign):
        for k, row in enumerate(full_rows(w, mu, sign)):
            total[k] = row if total[k] is None else added(total[k], row, 1)

    for mu in range(4):
        if mu == 0:
            ahead = signed(half(spinor(xtp), mu, -1), ahead_sign)
            behind = signed(half(spinor(xtm), mu, 1), behind_sign)
        elif mu == 1:
            ahead, behind = half(spinor(xzp), mu, -1), half(spinor(xzm), mu, 1)
        elif mu == 2:
            ahead = both(r_ahead, half(x, mu, -1), half(spinor(xrf), mu, -1))
            behind = both(r_behind, half(x, mu, 1), half(spinor(xrb), mu, 1))
        else:
            ahead, behind = y_up(half(x, mu, -1)), y_down(half(x, mu, 1))
        forward = colour(doubled(ul, mu), ahead)
        put(ws, mu, forward)
        gather(forward, mu, -1)
        gather(colour(doubled((utm, uzm, urm, uym)[mu], mu), behind, True), mu, 1)
    y = (
        jnp.stack([x[0][k] - HOPPING * total[k][0] for k in range(4)]),
        jnp.stack([x[1][k] - HOPPING * total[k][1] for k in range(4)]),
    )
    ys[0], ys[1] = y
    for mu in range(3):
        put(hy, mu, half(y, mu, 1))

    sent_spinor(hy.at[0], zero, every_z, hyn.at[0], edge_t, every_z, 3, t_behind)
    sent_spinor(hy.at[1], every_t, zero, hyn.at[1], every_t, edge_z, 3, z_behind)
    send(hy.at[2], hyn.at[2], r_prev)
    staged = len(locals_)
    spinor_boxes(hy.at[0], (tail_t, every_z), hyn.at[0], (head_t, every_z), 3, bring)
    spinor_boxes(hy.at[1], (every_t, tail_z), hyn.at[1], (every_t, head_z), 3, bring)

    for copy in remotes[first_remotes:link_remotes]:
        copy.wait_recv()

    for mu in (0, 1, 3):
        here = gauge(ul, mu)
        put(urp, mu, both(r_ahead, here, gauge(urf, mu)))
        put(urm, mu, both(r_behind, here, gauge(urb, mu)))
    put(edges, 2, both(r_behind, gauge(utp, 2), gauge(far, 0)))
    put(edges, 3, both(r_ahead, gauge(utm, 0), gauge(far, 1)))
    put(edges, 4, both(r_behind, gauge(uzp, 2), gauge(far, 2)))
    put(edges, 5, both(r_ahead, gauge(uzm, 1), gauge(far, 3)))
    put(edges, 6, y_down(gauge(utp, 3)))
    put(edges, 7, y_up(gauge(utm, 0)))
    put(edges, 8, y_down(gauge(uzp, 3)))
    put(edges, 9, y_up(gauge(uzm, 1)))
    put(edges, 10, y_down(gauge(urp, 3)))
    put(edges, 11, y_up(gauge(urm, 2)))

    slot_of = {(0, 1): 0, (1, 0): 1, (0, 2): 2, (2, 0): 3, (1, 2): 4, (2, 1): 5,
               (0, 3): 6, (3, 0): 7, (1, 3): 8, (3, 1): 9, (2, 3): 10, (3, 2): 11}
    plus = (utp, uzp, urp, uyp)
    minus = (utm, uzm, urm, uym)

    def paired(one, two):
        return both(lambda p, q: jnp.concatenate([p, q], 2), one, two)

    def swapped(value):
        return both(lambda v: jnp.concatenate([v[:, :, rows:], v[:, :, :rows]], 2), value)

    planes = [(mu, nu) for mu in range(4) for nu in range(mu + 1, 4)]
    for k, (mu, nu) in enumerate(planes):
        here = paired(gauge(ul, mu), gauge(ul, nu))
        ahead = paired(gauge(plus[mu], nu), gauge(plus[nu], mu))
        walk = product(here, ahead)
        upper = product(walk, swapped(walk), right_dagger=True)
        corner = paired(gauge(edges, slot_of[mu, nu]), gauge(edges, slot_of[nu, mu]))
        side = paired(gauge(minus[nu], mu), gauge(minus[mu], nu))
        back = paired(gauge(minus[nu], nu), gauge(minus[mu], mu))
        lower = product(
            product(here, corner, right_dagger=True), product(side, back, left_dagger=True)
        )
        fs[k] = nine(added(upper, lower, 1), PLAQUETTE)

    for copy in locals_[staged:]:
        copy.wait()
    for copy in remotes[link_remotes:]:
        copy.wait_recv()

    x = spinor(xs)
    y = spinor(ys)
    for mu in range(4):
        if mu == 3:
            ahead = y_up(half(y, 3, 1))
        elif mu == 2:
            ahead = both(r_ahead, gauge(hy, 2), gauge(hyn, 2))
        else:
            ahead = gauge(hyn, mu)
            if mu == 0:
                ahead = signed(ahead, ahead_sign)
        moved = colour(doubled(ul, mu), ahead)
        term = added(outer(gauge(ws, mu), half(y, mu, -1)), outer(moved, half(x, mu, 1)), 1)
        gs[mu] = nine(term, HOPPING)
        parts = gs[mu, :, pl.ds(0, rows)]
        for n in range(1, solves):
            parts = parts + gs[mu, :, pl.ds(n * rows, rows)]
        for k, plane in enumerate(planes):
            if mu in plane:
                parts = parts + fs[k, :, pl.ds(plane.index(mu) * rows, rows)]
        third = (parts[6] + parts[7] + parts[8]) / 3.0
        for k, (i, j) in enumerate(((0, 1), (0, 2), (1, 2))):
            force[mu, 0, i, j] = parts[k]
            force[mu, 0, j, i] = -parts[k]
            force[mu, 1, i, j] = parts[3 + k]
            force[mu, 1, j, i] = parts[3 + k]
        for i in range(3):
            force[mu, 0, i, i] = jnp.zeros_like(third)
            force[mu, 1, i, i] = parts[6 + i] - third

    for copy in remotes:
        copy.wait_send()


def on_device(sizes, links, solutions):
    whole = links.shape
    lanes = whole[-1]
    block = whole[4:6]
    rows = block[0] * block[1]
    links = links.reshape(*whole[:4], rows, lanes)
    n, c, s, a = solutions.shape[:4]
    solutions = solutions.reshape(n, c, s, a, rows, lanes)

    def vmem(*shape):
        return pltpu.VMEM(shape, jnp.float32)

    u = vmem(*links.shape)
    x = vmem(c, s, a, n * rows, lanes)
    unused = vmem(8, lanes) if sizes[2] == 2 else None
    small = links.shape[1:]
    h = vmem(3, c, 2, a, n * rows, lanes)
    out = pl.pallas_call(
        functools.partial(kernel, sizes, block),
        out_shape=jax.ShapeDtypeStruct(links.shape, jnp.float32),
        in_specs=[pl.BlockSpec(memory_space=pl.ANY)] * 2,
        out_specs=pl.BlockSpec(memory_space=pltpu.VMEM),
        scratch_shapes=[u] * 6 + [unused or u] + [u] * 4 + [vmem(12, *small), vmem(4, *small)]
        + [x] * 6 + [unused or x] + [x, h, h]
        + [vmem(4, c, 2, a, n * rows, lanes), vmem(6, 9, 2 * rows, lanes),
           vmem(4, 9, n * rows, lanes)]
        + [pltpu.SemaphoreType.DMA((LOCAL_COPIES,)), pltpu.SemaphoreType.DMA((REMOTE_COPIES,)),
           pltpu.SemaphoreType.DMA((REMOTE_COPIES,))],
        compiler_params=pltpu.CompilerParams(collective_id=0, has_side_effects=True),
    )(links, solutions)
    return out.reshape(whole)


def solution(mesh):
    sizes = tuple(mesh.shape[axis] for axis in AXES)
    spec = P(None, None, None, None, *AXES)
    return jax.shard_map(
        functools.partial(on_device, sizes), mesh=mesh, in_specs=(spec, spec), out_specs=spec,
        check_vma=False,
    )
```

```python
import functools

import jax
import jax.numpy as jnp
from jax import lax
from jax.experimental import pallas as pl
from jax.experimental.pallas import tpu as pltpu
from jax.sharding import PartitionSpec as P

Y_LEN = 64
HOPPING = 0.125
PLAQUETTE = 0.5
AXES = ("ta", "gz", "xy")
MESH = pl.DeviceIdType.MESH

SIGMA = (
    ((0, 0), (1, 0)),
    ((0, 1), (1, 3)),
    ((1, 1), (0, 1)),
    ((1, 2), (0, 0)),
)


def phased(value, power):
    re, im = value
    return ((re, im), (-im, re), (-re, -im), (im, -re))[power % 4]


def added(a, b, sign):
    if sign > 0:
        return a[0] + b[0], a[1] + b[1]
    return a[0] - b[0], a[1] - b[1]


def half(x, mu, sign):
    rows = []
    for s in range(2):
        column, power = SIGMA[mu][s]
        lower = phased((x[0][2 + column], x[1][2 + column]), power)
        rows.append(added((x[0][s], x[1][s]), lower, sign))
    return jnp.stack([rows[0][0], rows[1][0]]), jnp.stack([rows[0][1], rows[1][1]])


def full_rows(h, mu, sign):
    lower = [None, None]
    for s in range(2):
        column, power = SIGMA[mu][s]
        lower[column] = phased((h[0][s], h[1][s]), (-power if sign > 0 else 2 - power))
    return [(h[0][0], h[1][0]), (h[0][1], h[1][1])] + lower


def product(left, right, left_dagger=False, right_dagger=False):
    re = im = None
    for k in range(3):
        ar, ai = (left[0][k], left[1][k]) if left_dagger else (left[0][:, k], left[1][:, k])
        br, bi = (right[0][:, k], right[1][:, k]) if right_dagger else (right[0][k], right[1][k])
        ar, ai, br, bi = ar[:, None], ai[:, None], br[None], bi[None]
        rr, ii, ri, ir = ar * br, ai * bi, ar * bi, ai * br
        same = left_dagger == right_dagger
        re_k = rr - ii if same else rr + ii
        if left_dagger:
            im_k = -(ri + ir) if right_dagger else ri - ir
        else:
            im_k = ir - ri if right_dagger else ri + ir
        re = re_k if re is None else re + re_k
        im = im_k if im is None else im + im_k
    return re, im


def colour(u, h, dagger=False):
    re = im = None
    for k in range(3):
        ur, ui = (u[0][k], u[1][k]) if dagger else (u[0][:, k], u[1][:, k])
        ur, ui = ur[None], ui[None]
        hr, hi = h[0][:, k][:, None], h[1][:, k][:, None]
        if dagger:
            re_k, im_k = ur * hr + ui * hi, ur * hi - ui * hr
        else:
            re_k, im_k = ur * hr - ui * hi, ur * hi + ui * hr
        re = re_k if re is None else re + re_k
        im = im_k if im is None else im + im_k
    return re, im


def outer(f, g):
    re = im = None
    for s in range(2):
        fr, fi = f[0][s][:, None], f[1][s][:, None]
        gr, gi = g[0][s][None], g[1][s][None]
        re_s, im_s = fr * gr + fi * gi, fi * gr - fr * gi
        re = re_s if re is None else re + re_s
        im = im_s if im is None else im + im_s
    return re, im


def nine(m, scale):
    re, im = m
    pairs = ((0, 1), (0, 2), (1, 2))
    parts = [(re[i, j] - re[j, i]) * (0.5 * scale) for i, j in pairs]
    parts += [(im[i, j] + im[j, i]) * (0.5 * scale) for i, j in pairs]
    parts += [im[i, i] * scale for i in range(3)]
    return jnp.stack(parts)


def roll(value, by):
    lanes = value.shape[-1]
    return pltpu.roll(value, by % lanes, value.ndim - 1)


def y_shift(value, stride):
    lanes = value.shape[-1]
    at = lax.broadcasted_iota(jnp.int32, value.shape, value.ndim - 1) % Y_LEN
    if stride > 0:
        return jnp.where(at == Y_LEN - 1, roll(value, Y_LEN - 1), roll(value, lanes - 1))
    return jnp.where(at == 0, roll(value, lanes - Y_LEN + 1), roll(value, 1))


def r_ahead(here, ahead):
    lane = lax.broadcasted_iota(jnp.int32, here.shape, here.ndim - 1)
    return roll(jnp.where(lane < Y_LEN, ahead, here), here.shape[-1] - Y_LEN)


def r_behind(here, behind):
    lanes = here.shape[-1]
    lane = lax.broadcasted_iota(jnp.int32, here.shape, here.ndim - 1)
    return roll(jnp.where(lane >= lanes - Y_LEN, behind, here), Y_LEN)


def offsets(sizes):
    t, z, r = (1, 0, 0), (0, 1, 0), (0, 0, 1)
    steps = [t, z, r]
    steps += [(1, -1, 0), (1, 0, -1), (0, 1, -1)]
    both = steps + [tuple(-c for c in step) for step in steps]
    unique = []
    for step in both:
        seat = tuple(c % n for c, n in zip(step, sizes))
        if seat not in unique:
            unique.append(seat)
    return unique


LOCAL_COPIES = 64
REMOTE_COPIES = 96


def kernel(sizes, block, links, solutions, force, *refs):
    (ul, utp, utm, uzp, uzm, urf, urb, urp, urm, uyp, uym, edges, far, xs,
     hx, hxn, xrf, xrb, ys, hy, hyn, ws, fs, gs, local, sends, recvs) = refs
    blocks_t, blocks_z = block
    rows, lanes = ul.shape[-2:]
    solves = xs.shape[-2] // rows
    last_t, last_z = blocks_t - 1, blocks_z - 1
    one_ring = sizes[2] == 2
    if one_ring:
        urb, xrb = urf, xrf
    me = [lax.axis_index(axis) for axis in AXES]

    def seat(step):
        return {
            axis: m if c % n == 0 else lax.rem(m + (c % n), n)
            for axis, m, c, n in zip(AXES, me, step, sizes)
        }

    def spinor(ref):
        return ref[0], ref[1]

    def gauge(ref, mu):
        return ref[mu, 0], ref[mu, 1]

    def put(ref, mu, value):
        ref[mu, 0], ref[mu, 1] = value

    def two(ref, mu):
        return ref.at[mu, :, pl.ds(0, 2)]

    def third(ref, mu):
        re, im = gauge(ref, mu)
        for c in range(3):
            p, q = (c + 1) % 3, (c + 2) % 3
            a, b, f, g = (0, p), (1, q), (0, q), (1, p)
            ref[mu, 0, 2, c] = re[a] * re[b] - im[a] * im[b] - re[f] * re[g] + im[f] * im[g]
            ref[mu, 1, 2, c] = re[f] * im[g] + im[f] * re[g] - re[a] * im[b] - im[a] * re[b]

    every_t, every_z = (0, blocks_t), (0, blocks_z)

    def runs(box_t, box_z):
        (t, many_t), (z, many_z) = box_t, box_z
        if many_z == blocks_z:
            return [(t * blocks_z, many_t * blocks_z)]
        return [((t + k) * blocks_z + z, many_z) for k in range(many_t)]

    head_t, tail_t, zero, edge_t = (0, last_t), (1, last_t), (0, 1), (last_t, 1)
    head_z, tail_z, edge_z = (0, last_z), (1, last_z), (last_z, 1)

    locals_, remotes = [], []

    def bring(source, target):
        copy = pltpu.make_async_copy(source, target, local.at[len(locals_)])
        copy.start()
        locals_.append(copy)

    def send(source, target, step):
        k = len(remotes)
        copy = pltpu.make_async_remote_copy(
            src_ref=source, dst_ref=target, send_sem=sends.at[k], recv_sem=recvs.at[k],
            device_id=seat(step), device_id_type=MESH,
        )
        copy.start()
        remotes.append(copy)

    def boxes(source, from_box, target, to_box, lead, one):
        everything = (slice(None),) * lead
        for (a, n), (b, _) in zip(runs(*from_box), runs(*to_box)):
            one(source.at[(*everything, pl.ds(a, n))], target.at[(*everything, pl.ds(b, n))])

    def spinor_boxes(source, from_box, target, to_box, lead, one):
        everything = (slice(None),) * lead
        for s in range(solves):
            for (a, n), (b, _) in zip(runs(*from_box), runs(*to_box)):
                one(
                    source.at[(*everything, pl.ds(s * rows + a, n))],
                    target.at[(*everything, pl.ds(s * rows + b, n))],
                )

    bring(links, ul)
    for n in range(solves):
        bring(solutions.at[n], xs.at[:, :, :, pl.ds(n * rows, rows)])
    first_locals = len(locals_)
    boxes(links, (tail_t, every_z), utp, (head_t, every_z), 4, bring)
    boxes(links, (head_t, every_z), utm, (tail_t, every_z), 4, bring)
    boxes(links, (every_t, tail_z), uzp, (every_t, head_z), 4, bring)
    boxes(links, (every_t, head_z), uzm, (every_t, tail_z), 4, bring)
    boxes(links.at[1], (tail_t, head_z), edges.at[0], (head_t, tail_z), 3, bring)
    boxes(links.at[0], (head_t, tail_z), edges.at[1], (tail_t, head_z), 3, bring)

    barrier = pltpu.get_barrier_semaphore()
    peers = offsets(sizes)
    for step in peers:
        pl.semaphore_signal(barrier, inc=1, device_id=seat(step), device_id_type=MESH)
    for copy in locals_[:first_locals]:
        copy.wait()
    x = spinor(xs)
    for k, (mu, sign) in enumerate(((0, -1), (0, 1), (1, -1), (1, 1))):
        put(hx, k, half(x, mu, sign))
    pl.semaphore_wait(barrier, len(peers))

    t_ahead, t_behind, z_ahead, z_behind = (1, 0, 0), (-1, 0, 0), (0, 1, 0), (0, -1, 0)
    r_next, r_prev = (0, 0, 1), (0, 0, -1)

    def sent(source, from_t, from_z, target, to_t, to_z, lead, step):
        boxes(source, (from_t, from_z), target, (to_t, to_z), lead,
              lambda a, b: send(a, b, step))

    def sent_spinor(source, from_t, from_z, target, to_t, to_z, lead, step):
        spinor_boxes(source, (from_t, from_z), target, (to_t, to_z), lead,
                     lambda a, b: send(a, b, step))

    sent_spinor(hx.at[0], zero, every_z, hxn.at[0], edge_t, every_z, 3, t_behind)
    sent_spinor(hx.at[1], edge_t, every_z, hxn.at[1], zero, every_z, 3, t_ahead)
    sent_spinor(hx.at[2], every_t, zero, hxn.at[2], every_t, edge_z, 3, z_behind)
    sent_spinor(hx.at[3], every_t, edge_z, hxn.at[3], every_t, zero, 3, z_ahead)
    sent(two(ul, 0), edge_t, every_z, two(utm, 0), zero, every_z, 3, t_ahead)
    sent(two(ul, 1), every_t, edge_z, two(uzm, 1), every_t, zero, 3, z_ahead)
    send(xs, xrf, r_prev)
    if not one_ring:
        send(xs, xrb, r_next)
    send(ul.at[2], urb.at[2], r_prev if one_ring else r_next)
    first_remotes = len(remotes)
    later, other = pl.ds(1, 3), pl.ds(2, 2)
    sent(two(ul, later), zero, every_z, two(utp, later), edge_t, every_z, 4, t_behind)
    sent(two(ul, later), edge_t, every_z, two(utm, later), zero, every_z, 4, t_ahead)
    sent(two(ul, 0), every_t, zero, two(uzp, 0), every_t, edge_z, 3, z_behind)
    sent(two(ul, other), every_t, zero, two(uzp, other), every_t, edge_z, 4, z_behind)
    sent(two(ul, 0), every_t, edge_z, two(uzm, 0), every_t, zero, 3, z_ahead)
    sent(two(ul, other), every_t, edge_z, two(uzm, other), every_t, zero, 4, z_ahead)
    sent(two(ul, 1), tail_t, edge_z, two(edges, 0), head_t, zero, 3, z_ahead)
    sent(two(ul, 1), zero, edge_z, two(edges, 0), edge_t, zero, 3, (-1, 1, 0))
    sent(two(ul, 1), zero, head_z, two(edges, 0), edge_t, tail_z, 3, t_behind)
    sent(two(ul, 0), edge_t, tail_z, two(edges, 1), zero, head_z, 3, t_ahead)
    sent(two(ul, 0), edge_t, zero, two(edges, 1), zero, edge_z, 3, (1, -1, 0))
    sent(two(ul, 0), head_t, zero, two(edges, 1), tail_t, edge_z, 3, z_behind)
    sent(two(ul, 2), zero, every_z, two(far, 0), edge_t, every_z, 3, (-1, 0, 1))
    sent(two(ul, 0), edge_t, every_z, two(far, 1), zero, every_z, 3, (1, 0, -1))
    sent(two(ul, 2), every_t, zero, two(far, 2), every_t, edge_z, 3, (0, -1, 1))
    sent(two(ul, 1), every_t, edge_z, two(far, 3), every_t, zero, 3, (0, 1, -1))
    sent(two(ul, 2), tail_t, every_z, two(far, 0), head_t, every_z, 3, r_next)
    sent(two(ul, 0), head_t, every_z, two(far, 1), tail_t, every_z, 3, r_prev)
    sent(two(ul, 2), every_t, tail_z, two(far, 2), every_t, head_z, 3, r_next)
    sent(two(ul, 1), every_t, head_z, two(far, 3), every_t, tail_z, 3, r_prev)
    send(ul.at[pl.ds(0, 2)], urf.at[pl.ds(0, 2)], r_prev)
    send(ul.at[3], urf.at[3], r_prev)
    if not one_ring:
        send(ul.at[pl.ds(0, 2)], urb.at[pl.ds(0, 2)], r_next)
        send(ul.at[3], urb.at[3], r_next)
    link_remotes = len(remotes)
    spinor_boxes(hx.at[0], (tail_t, every_z), hxn.at[0], (head_t, every_z), 3, bring)
    spinor_boxes(hx.at[1], (head_t, every_z), hxn.at[1], (tail_t, every_z), 3, bring)
    spinor_boxes(hx.at[2], (every_t, tail_z), hxn.at[2], (every_t, head_z), 3, bring)
    spinor_boxes(hx.at[3], (every_t, head_z), hxn.at[3], (every_t, tail_z), 3, bring)

    def doubled(ref, mu):
        re, im = gauge(ref, mu)
        return jnp.concatenate([re] * solves, 2), jnp.concatenate([im] * solves, 2)

    def both(f, *values):
        return tuple(f(*parts) for parts in zip(*values))

    index = lax.broadcasted_iota(jnp.int32, (solves * rows, lanes), 0)
    index = (index // blocks_z) % blocks_t
    wraps_ahead = (index == last_t) & (me[0] == sizes[0] - 1)
    wraps_behind = (index == 0) & (me[0] == 0)
    ahead_sign = jnp.where(wraps_ahead, -1.0, 1.0)
    behind_sign = jnp.where(wraps_behind, -1.0, 1.0)

    def signed(h, sign):
        return both(lambda v: v * sign, h)

    def y_up(value):
        return both(lambda v: y_shift(v, 1), value)

    def y_down(value):
        return both(lambda v: y_shift(v, -1), value)

    for mu in range(4):
        here = gauge(ul, mu)
        if mu < 3:
            put(uyp, mu, y_up(here))
        put(uym, mu, y_down(here))

    for copy in locals_[first_locals:]:
        copy.wait()
    for copy in remotes[:first_remotes]:
        copy.wait_recv()

    third(utm, 0)
    third(uzm, 1)
    put(urm, 2, both(r_behind, gauge(ul, 2), gauge(urb, 2)))

    x = spinor(xs)
    total = [None] * 4

    def gather(w, mu, sign):
        for k, row in enumerate(full_rows(w, mu, sign)):
            total[k] = row if total[k] is None else added(total[k], row, 1)

    for mu in range(4):
        if mu == 0:
            ahead = signed(gauge(hxn, 0), ahead_sign)
            behind = signed(gauge(hxn, 1), behind_sign)
        elif mu == 1:
            ahead, behind = gauge(hxn, 2), gauge(hxn, 3)
        elif mu == 2:
            ahead = both(r_ahead, half(x, mu, -1), half(spinor(xrf), mu, -1))
            behind = both(r_behind, half(x, mu, 1), half(spinor(xrb), mu, 1))
        else:
            ahead, behind = y_up(half(x, mu, -1)), y_down(half(x, mu, 1))
        forward = colour(doubled(ul, mu), ahead)
        put(ws, mu, forward)
        gather(forward, mu, -1)
        gather(colour(doubled((utm, uzm, urm, uym)[mu], mu), behind, True), mu, 1)
    y = (
        jnp.stack([x[0][k] - HOPPING * total[k][0] for k in range(4)]),
        jnp.stack([x[1][k] - HOPPING * total[k][1] for k in range(4)]),
    )
    ys[0], ys[1] = y
    for mu in range(3):
        put(hy, mu, half(y, mu, 1))

    sent_spinor(hy.at[0], zero, every_z, hyn.at[0], edge_t, every_z, 3, t_behind)
    sent_spinor(hy.at[1], every_t, zero, hyn.at[1], every_t, edge_z, 3, z_behind)
    send(hy.at[2], hyn.at[2], r_prev)
    staged = len(locals_)
    spinor_boxes(hy.at[0], (tail_t, every_z), hyn.at[0], (head_t, every_z), 3, bring)
    spinor_boxes(hy.at[1], (every_t, tail_z), hyn.at[1], (every_t, head_z), 3, bring)

    for copy in remotes[first_remotes:link_remotes]:
        copy.wait_recv()

    for mu in (1, 2, 3):
        third(utp, mu)
        third(utm, mu)
    for mu in (0, 2, 3):
        third(uzp, mu)
        third(uzm, mu)
    for k in range(2):
        third(edges, k)
    for k in range(4):
        third(far, k)
    for mu in (0, 1, 3):
        here = gauge(ul, mu)
        put(urp, mu, both(r_ahead, here, gauge(urf, mu)))
        put(urm, mu, both(r_behind, here, gauge(urb, mu)))
    put(edges, 2, both(r_behind, gauge(utp, 2), gauge(far, 0)))
    put(edges, 3, both(r_ahead, gauge(utm, 0), gauge(far, 1)))
    put(edges, 4, both(r_behind, gauge(uzp, 2), gauge(far, 2)))
    put(edges, 5, both(r_ahead, gauge(uzm, 1), gauge(far, 3)))
    put(edges, 6, y_down(gauge(utp, 3)))
    put(edges, 7, y_up(gauge(utm, 0)))
    put(edges, 8, y_down(gauge(uzp, 3)))
    put(edges, 9, y_up(gauge(uzm, 1)))
    put(edges, 10, y_down(gauge(urp, 3)))
    put(edges, 11, y_up(gauge(urm, 2)))

    slot_of = {(0, 1): 0, (1, 0): 1, (0, 2): 2, (2, 0): 3, (1, 2): 4, (2, 1): 5,
               (0, 3): 6, (3, 0): 7, (1, 3): 8, (3, 1): 9, (2, 3): 10, (3, 2): 11}
    plus = (utp, uzp, urp, uyp)
    minus = (utm, uzm, urm, uym)

    def paired(one, two):
        return both(lambda p, q: jnp.concatenate([p, q], 2), one, two)

    def swapped(value):
        return both(lambda v: jnp.concatenate([v[:, :, rows:], v[:, :, :rows]], 2), value)

    planes = [(mu, nu) for mu in range(4) for nu in range(mu + 1, 4)]
    for k, (mu, nu) in enumerate(planes):
        here = paired(gauge(ul, mu), gauge(ul, nu))
        ahead = paired(gauge(plus[mu], nu), gauge(plus[nu], mu))
        walk = product(here, ahead)
        upper = product(walk, swapped(walk), right_dagger=True)
        corner = paired(gauge(edges, slot_of[mu, nu]), gauge(edges, slot_of[nu, mu]))
        side = paired(gauge(minus[nu], mu), gauge(minus[mu], nu))
        back = paired(gauge(minus[nu], nu), gauge(minus[mu], mu))
        lower = product(
            product(here, corner, right_dagger=True), product(side, back, left_dagger=True)
        )
        fs[k] = nine(added(upper, lower, 1), PLAQUETTE)

    for copy in locals_[staged:]:
        copy.wait()
    for copy in remotes[link_remotes:]:
        copy.wait_recv()

    x = spinor(xs)
    y = spinor(ys)
    for mu in range(4):
        if mu == 3:
            ahead = y_up(half(y, 3, 1))
        elif mu == 2:
            ahead = both(r_ahead, gauge(hy, 2), gauge(hyn, 2))
        else:
            ahead = gauge(hyn, mu)
            if mu == 0:
                ahead = signed(ahead, ahead_sign)
        moved = colour(doubled(ul, mu), ahead)
        term = added(outer(gauge(ws, mu), half(y, mu, -1)), outer(moved, half(x, mu, 1)), 1)
        gs[mu] = nine(term, HOPPING)
        parts = gs[mu, :, pl.ds(0, rows)]
        for n in range(1, solves):
            parts = parts + gs[mu, :, pl.ds(n * rows, rows)]
        for k, plane in enumerate(planes):
            if mu in plane:
                parts = parts + fs[k, :, pl.ds(plane.index(mu) * rows, rows)]
        mean = (parts[6] + parts[7] + parts[8]) / 3.0
        for k, (i, j) in enumerate(((0, 1), (0, 2), (1, 2))):
            force[mu, 0, i, j] = parts[k]
            force[mu, 0, j, i] = -parts[k]
            force[mu, 1, i, j] = parts[3 + k]
            force[mu, 1, j, i] = parts[3 + k]
        for i in range(3):
            force[mu, 0, i, i] = jnp.zeros_like(mean)
            force[mu, 1, i, i] = parts[6 + i] - mean

    for copy in remotes:
        copy.wait_send()


def on_device(sizes, links, solutions):
    whole = links.shape
    lanes = whole[-1]
    block = whole[4:6]
    rows = block[0] * block[1]
    links = links.reshape(*whole[:4], rows, lanes)
    n, c, s, a = solutions.shape[:4]
    solutions = solutions.reshape(n, c, s, a, rows, lanes)

    def vmem(*shape):
        return pltpu.VMEM(shape, jnp.float32)

    u = vmem(*links.shape)
    x = vmem(c, s, a, n * rows, lanes)
    unused = vmem(8, lanes) if sizes[2] == 2 else None
    small = links.shape[1:]
    h = vmem(3, c, 2, a, n * rows, lanes)
    h4 = vmem(4, c, 2, a, n * rows, lanes)
    out = pl.pallas_call(
        functools.partial(kernel, sizes, block),
        out_shape=jax.ShapeDtypeStruct(links.shape, jnp.float32),
        in_specs=[pl.BlockSpec(memory_space=pl.ANY)] * 2,
        out_specs=pl.BlockSpec(memory_space=pltpu.VMEM),
        scratch_shapes=[u] * 6 + [unused or u] + [u] * 4 + [vmem(12, *small), vmem(4, *small)]
        + [x, h4, h4, x, unused or x, x, h, h]
        + [vmem(4, c, 2, a, n * rows, lanes), vmem(6, 9, 2 * rows, lanes),
           vmem(4, 9, n * rows, lanes)]
        + [pltpu.SemaphoreType.DMA((LOCAL_COPIES,)), pltpu.SemaphoreType.DMA((REMOTE_COPIES,)),
           pltpu.SemaphoreType.DMA((REMOTE_COPIES,))],
        compiler_params=pltpu.CompilerParams(collective_id=0, has_side_effects=True),
    )(links, solutions)
    return out.reshape(whole)


def solution(mesh):
    sizes = tuple(mesh.shape[axis] for axis in AXES)
    spec = P(None, None, None, None, *AXES)
    return jax.shard_map(
        functools.partial(on_device, sizes), mesh=mesh, in_specs=(spec, spec), out_specs=spec,
        check_vma=False,
    )
```

```python
import functools

import jax
import jax.numpy as jnp
from jax import lax
from jax.experimental import pallas as pl
from jax.experimental.pallas import tpu as pltpu
from jax.sharding import PartitionSpec as P

Y_LEN = 64
HOPPING = 0.125
PLAQUETTE = 0.5
AXES = ("ta", "gz", "xy")
MESH = pl.DeviceIdType.MESH

SIGMA = (
    ((0, 0), (1, 0)),
    ((0, 1), (1, 3)),
    ((1, 1), (0, 1)),
    ((1, 2), (0, 0)),
)


def phased(value, power):
    re, im = value
    return ((re, im), (-im, re), (-re, -im), (im, -re))[power % 4]


def added(a, b, sign):
    if sign > 0:
        return a[0] + b[0], a[1] + b[1]
    return a[0] - b[0], a[1] - b[1]


def half(x, mu, sign):
    rows = []
    for s in range(2):
        column, power = SIGMA[mu][s]
        lower = phased((x[0][2 + column], x[1][2 + column]), power)
        rows.append(added((x[0][s], x[1][s]), lower, sign))
    return jnp.stack([rows[0][0], rows[1][0]]), jnp.stack([rows[0][1], rows[1][1]])


def full_rows(h, mu, sign):
    lower = [None, None]
    for s in range(2):
        column, power = SIGMA[mu][s]
        lower[column] = phased((h[0][s], h[1][s]), (-power if sign > 0 else 2 - power))
    return [(h[0][0], h[1][0]), (h[0][1], h[1][1])] + lower


def product(left, right, left_dagger=False, right_dagger=False):
    re = im = None
    for k in range(3):
        ar, ai = (left[0][k], left[1][k]) if left_dagger else (left[0][:, k], left[1][:, k])
        br, bi = (right[0][:, k], right[1][:, k]) if right_dagger else (right[0][k], right[1][k])
        ar, ai, br, bi = ar[:, None], ai[:, None], br[None], bi[None]
        rr, ii, ri, ir = ar * br, ai * bi, ar * bi, ai * br
        same = left_dagger == right_dagger
        re_k = rr - ii if same else rr + ii
        if left_dagger:
            im_k = -(ri + ir) if right_dagger else ri - ir
        else:
            im_k = ir - ri if right_dagger else ri + ir
        re = re_k if re is None else re + re_k
        im = im_k if im is None else im + im_k
    return re, im


def colour(u, h, dagger=False):
    re = im = None
    for k in range(3):
        ur, ui = (u[0][k], u[1][k]) if dagger else (u[0][:, k], u[1][:, k])
        ur, ui = ur[None], ui[None]
        hr, hi = h[0][:, k][:, None], h[1][:, k][:, None]
        if dagger:
            re_k, im_k = ur * hr + ui * hi, ur * hi - ui * hr
        else:
            re_k, im_k = ur * hr - ui * hi, ur * hi + ui * hr
        re = re_k if re is None else re + re_k
        im = im_k if im is None else im + im_k
    return re, im


def outer(f, g):
    re = im = None
    for s in range(2):
        fr, fi = f[0][s][:, None], f[1][s][:, None]
        gr, gi = g[0][s][None], g[1][s][None]
        re_s, im_s = fr * gr + fi * gi, fi * gr - fr * gi
        re = re_s if re is None else re + re_s
        im = im_s if im is None else im + im_s
    return re, im


def nine(m, scale):
    re, im = m
    pairs = ((0, 1), (0, 2), (1, 2))
    parts = [(re[i, j] - re[j, i]) * (0.5 * scale) for i, j in pairs]
    parts += [(im[i, j] + im[j, i]) * (0.5 * scale) for i, j in pairs]
    parts += [im[i, i] * scale for i in range(3)]
    return jnp.stack(parts)


def roll(value, by):
    lanes = value.shape[-1]
    return pltpu.roll(value, by % lanes, value.ndim - 1)


def y_shift(value, stride):
    lanes = value.shape[-1]
    at = lax.broadcasted_iota(jnp.int32, value.shape, value.ndim - 1) % Y_LEN
    if stride > 0:
        return jnp.where(at == Y_LEN - 1, roll(value, Y_LEN - 1), roll(value, lanes - 1))
    return jnp.where(at == 0, roll(value, lanes - Y_LEN + 1), roll(value, 1))


def r_ahead(here, ahead):
    lane = lax.broadcasted_iota(jnp.int32, here.shape, here.ndim - 1)
    return roll(jnp.where(lane < Y_LEN, ahead, here), here.shape[-1] - Y_LEN)


def r_behind(here, behind):
    lanes = here.shape[-1]
    lane = lax.broadcasted_iota(jnp.int32, here.shape, here.ndim - 1)
    return roll(jnp.where(lane >= lanes - Y_LEN, behind, here), Y_LEN)


def offsets(sizes):
    t, z, r = (1, 0, 0), (0, 1, 0), (0, 0, 1)
    steps = [t, z, r]
    steps += [(1, -1, 0), (1, 0, -1), (0, 1, -1)]
    both = steps + [tuple(-c for c in step) for step in steps]
    unique = []
    for step in both:
        seat = tuple(c % n for c, n in zip(step, sizes))
        if seat not in unique:
            unique.append(seat)
    return unique


LOCAL_COPIES = 64
REMOTE_COPIES = 96


def kernel(sizes, block, links, solutions, force, *refs):
    (ul, utp, utm, uzp, uzm, urf, urb, urp, urm, uyp, uym, edges, far, xs,
     hx, hxn, xrf, xrb, ys, hy, hyn, ws, fs, gs, local, sends, recvs) = refs
    blocks_t, blocks_z = block
    rows, lanes = ul.shape[-2:]
    solves = xs.shape[-2] // rows
    last_t, last_z = blocks_t - 1, blocks_z - 1
    one_ring = sizes[2] == 2
    if one_ring:
        urb, xrb = urf, xrf
    me = [lax.axis_index(axis) for axis in AXES]

    def seat(step):
        return {
            axis: m if c % n == 0 else lax.rem(m + (c % n), n)
            for axis, m, c, n in zip(AXES, me, step, sizes)
        }

    def spinor(ref):
        return ref[0], ref[1]

    def gauge(ref, mu):
        return ref[mu, 0], ref[mu, 1]

    def put(ref, mu, value):
        ref[mu, 0], ref[mu, 1] = value

    def two(ref, mu):
        return ref.at[mu, :, pl.ds(0, 2)]

    def third(ref, mu):
        re, im = gauge(ref, mu)
        for c in range(3):
            p, q = (c + 1) % 3, (c + 2) % 3
            a, b, f, g = (0, p), (1, q), (0, q), (1, p)
            ref[mu, 0, 2, c] = re[a] * re[b] - im[a] * im[b] - re[f] * re[g] + im[f] * im[g]
            ref[mu, 1, 2, c] = re[f] * im[g] + im[f] * re[g] - re[a] * im[b] - im[a] * re[b]

    def moved_rows(ref, mu, from_box, slot, to_box):
        for (a, n), (b, _) in zip(runs(*from_box), runs(*to_box)):
            for part in range(2):
                block = ref[mu, part, pl.ds(0, 2), :, pl.ds(a, n)]
                edges[slot, part, pl.ds(0, 2), :, pl.ds(b, n)] = block

    every_t, every_z = (0, blocks_t), (0, blocks_z)

    def runs(box_t, box_z):
        (t, many_t), (z, many_z) = box_t, box_z
        if many_z == blocks_z:
            return [(t * blocks_z, many_t * blocks_z)]
        return [((t + k) * blocks_z + z, many_z) for k in range(many_t)]

    head_t, tail_t, zero, edge_t = (0, last_t), (1, last_t), (0, 1), (last_t, 1)
    head_z, tail_z, edge_z = (0, last_z), (1, last_z), (last_z, 1)

    locals_, remotes = [], []

    def bring(source, target):
        copy = pltpu.make_async_copy(source, target, local.at[len(locals_)])
        copy.start()
        locals_.append(copy)

    def send(source, target, step):
        k = len(remotes)
        copy = pltpu.make_async_remote_copy(
            src_ref=source, dst_ref=target, send_sem=sends.at[k], recv_sem=recvs.at[k],
            device_id=seat(step), device_id_type=MESH,
        )
        copy.start()
        remotes.append(copy)

    def boxes(source, from_box, target, to_box, lead, one):
        everything = (slice(None),) * lead
        for (a, n), (b, _) in zip(runs(*from_box), runs(*to_box)):
            one(source.at[(*everything, pl.ds(a, n))], target.at[(*everything, pl.ds(b, n))])

    def spinor_boxes(source, from_box, target, to_box, lead, one):
        everything = (slice(None),) * lead
        for s in range(solves):
            for (a, n), (b, _) in zip(runs(*from_box), runs(*to_box)):
                one(
                    source.at[(*everything, pl.ds(s * rows + a, n))],
                    target.at[(*everything, pl.ds(s * rows + b, n))],
                )

    bring(links, ul)
    for n in range(solves):
        bring(solutions.at[n], xs.at[:, :, :, pl.ds(n * rows, rows)])
    first_locals = len(locals_)
    boxes(links, (tail_t, every_z), utp, (head_t, every_z), 4, bring)
    boxes(links, (head_t, every_z), utm, (tail_t, every_z), 4, bring)
    boxes(links, (every_t, tail_z), uzp, (every_t, head_z), 4, bring)
    boxes(links, (every_t, head_z), uzm, (every_t, tail_z), 4, bring)
    boxes(links.at[1], (tail_t, head_z), edges.at[0], (head_t, tail_z), 3, bring)
    boxes(links.at[0], (head_t, tail_z), edges.at[1], (tail_t, head_z), 3, bring)

    barrier = pltpu.get_barrier_semaphore()
    peers = offsets(sizes)
    for step in peers:
        pl.semaphore_signal(barrier, inc=1, device_id=seat(step), device_id_type=MESH)
    for copy in locals_[:first_locals]:
        copy.wait()
    x = spinor(xs)
    for k, (mu, sign) in enumerate(((0, -1), (0, 1), (1, -1), (1, 1))):
        put(hx, k, half(x, mu, sign))
    pl.semaphore_wait(barrier, len(peers))

    t_ahead, t_behind, z_ahead, z_behind = (1, 0, 0), (-1, 0, 0), (0, 1, 0), (0, -1, 0)
    r_next, r_prev = (0, 0, 1), (0, 0, -1)

    def sent(source, from_t, from_z, target, to_t, to_z, lead, step):
        boxes(source, (from_t, from_z), target, (to_t, to_z), lead,
              lambda a, b: send(a, b, step))

    def sent_spinor(source, from_t, from_z, target, to_t, to_z, lead, step):
        spinor_boxes(source, (from_t, from_z), target, (to_t, to_z), lead,
                     lambda a, b: send(a, b, step))

    sent_spinor(hx.at[0], zero, every_z, hxn.at[0], edge_t, every_z, 3, t_behind)
    sent_spinor(hx.at[1], edge_t, every_z, hxn.at[1], zero, every_z, 3, t_ahead)
    sent_spinor(hx.at[2], every_t, zero, hxn.at[2], every_t, edge_z, 3, z_behind)
    sent_spinor(hx.at[3], every_t, edge_z, hxn.at[3], every_t, zero, 3, z_ahead)
    sent(two(ul, 0), edge_t, every_z, two(utm, 0), zero, every_z, 3, t_ahead)
    sent(two(ul, 1), every_t, edge_z, two(uzm, 1), every_t, zero, 3, z_ahead)
    send(xs, xrf, r_prev)
    if not one_ring:
        send(xs, xrb, r_next)
    send(ul.at[2], urb.at[2], r_prev if one_ring else r_next)
    first_remotes = len(remotes)
    later, other = pl.ds(1, 3), pl.ds(2, 2)
    sent(two(ul, later), zero, every_z, two(utp, later), edge_t, every_z, 4, t_behind)
    sent(two(ul, later), edge_t, every_z, two(utm, later), zero, every_z, 4, t_ahead)
    sent(two(ul, 0), every_t, zero, two(uzp, 0), every_t, edge_z, 3, z_behind)
    sent(two(ul, other), every_t, zero, two(uzp, other), every_t, edge_z, 4, z_behind)
    sent(two(ul, 0), every_t, edge_z, two(uzm, 0), every_t, zero, 3, z_ahead)
    sent(two(ul, other), every_t, edge_z, two(uzm, other), every_t, zero, 4, z_ahead)
    sent(two(ul, 1), zero, edge_z, two(edges, 0), edge_t, zero, 3, (-1, 1, 0))
    sent(two(ul, 0), edge_t, zero, two(edges, 1), zero, edge_z, 3, (1, -1, 0))
    sent(two(ul, 2), zero, every_z, two(far, 0), edge_t, every_z, 3, (-1, 0, 1))
    sent(two(ul, 0), edge_t, every_z, two(far, 1), zero, every_z, 3, (1, 0, -1))
    sent(two(ul, 2), every_t, zero, two(far, 2), every_t, edge_z, 3, (0, -1, 1))
    sent(two(ul, 1), every_t, edge_z, two(far, 3), every_t, zero, 3, (0, 1, -1))
    sent(two(ul, 2), tail_t, every_z, two(far, 0), head_t, every_z, 3, r_next)
    sent(two(ul, 0), head_t, every_z, two(far, 1), tail_t, every_z, 3, r_prev)
    sent(two(ul, 2), every_t, tail_z, two(far, 2), every_t, head_z, 3, r_next)
    sent(two(ul, 1), every_t, head_z, two(far, 3), every_t, tail_z, 3, r_prev)
    send(ul.at[pl.ds(0, 2)], urf.at[pl.ds(0, 2)], r_prev)
    send(ul.at[3], urf.at[3], r_prev)
    if not one_ring:
        send(ul.at[pl.ds(0, 2)], urb.at[pl.ds(0, 2)], r_next)
        send(ul.at[3], urb.at[3], r_next)
    link_remotes = len(remotes)
    spinor_boxes(hx.at[0], (tail_t, every_z), hxn.at[0], (head_t, every_z), 3, bring)
    spinor_boxes(hx.at[1], (head_t, every_z), hxn.at[1], (tail_t, every_z), 3, bring)
    spinor_boxes(hx.at[2], (every_t, tail_z), hxn.at[2], (every_t, head_z), 3, bring)
    spinor_boxes(hx.at[3], (every_t, head_z), hxn.at[3], (every_t, tail_z), 3, bring)

    def doubled(ref, mu):
        re, im = gauge(ref, mu)
        return jnp.concatenate([re] * solves, 2), jnp.concatenate([im] * solves, 2)

    def both(f, *values):
        return tuple(f(*parts) for parts in zip(*values))

    index = lax.broadcasted_iota(jnp.int32, (solves * rows, lanes), 0)
    index = (index // blocks_z) % blocks_t
    wraps_ahead = (index == last_t) & (me[0] == sizes[0] - 1)
    wraps_behind = (index == 0) & (me[0] == 0)
    ahead_sign = jnp.where(wraps_ahead, -1.0, 1.0)
    behind_sign = jnp.where(wraps_behind, -1.0, 1.0)

    def signed(h, sign):
        return both(lambda v: v * sign, h)

    def y_up(value):
        return both(lambda v: y_shift(v, 1), value)

    def y_down(value):
        return both(lambda v: y_shift(v, -1), value)

    for mu in range(4):
        here = gauge(ul, mu)
        if mu < 3:
            put(uyp, mu, y_up(here))
        put(uym, mu, y_down(here))

    for copy in locals_[first_locals:]:
        copy.wait()
    for copy in remotes[:first_remotes]:
        copy.wait_recv()

    third(utm, 0)
    third(uzm, 1)
    put(urm, 2, both(r_behind, gauge(ul, 2), gauge(urb, 2)))

    x = spinor(xs)
    total = [None] * 4

    def gather(w, mu, sign):
        for k, row in enumerate(full_rows(w, mu, sign)):
            total[k] = row if total[k] is None else added(total[k], row, 1)

    for mu in range(4):
        if mu == 0:
            ahead = signed(gauge(hxn, 0), ahead_sign)
            behind = signed(gauge(hxn, 1), behind_sign)
        elif mu == 1:
            ahead, behind = gauge(hxn, 2), gauge(hxn, 3)
        elif mu == 2:
            ahead = both(r_ahead, half(x, mu, -1), half(spinor(xrf), mu, -1))
            behind = both(r_behind, half(x, mu, 1), half(spinor(xrb), mu, 1))
        else:
            ahead, behind = y_up(half(x, mu, -1)), y_down(half(x, mu, 1))
        forward = colour(doubled(ul, mu), ahead)
        put(ws, mu, forward)
        gather(forward, mu, -1)
        gather(colour(doubled((utm, uzm, urm, uym)[mu], mu), behind, True), mu, 1)
    y = (
        jnp.stack([x[0][k] - HOPPING * total[k][0] for k in range(4)]),
        jnp.stack([x[1][k] - HOPPING * total[k][1] for k in range(4)]),
    )
    ys[0], ys[1] = y
    for mu in range(3):
        put(hy, mu, half(y, mu, 1))

    sent_spinor(hy.at[0], zero, every_z, hyn.at[0], edge_t, every_z, 3, t_behind)
    sent_spinor(hy.at[1], every_t, zero, hyn.at[1], every_t, edge_z, 3, z_behind)
    send(hy.at[2], hyn.at[2], r_prev)
    staged = len(locals_)
    spinor_boxes(hy.at[0], (tail_t, every_z), hyn.at[0], (head_t, every_z), 3, bring)
    spinor_boxes(hy.at[1], (every_t, tail_z), hyn.at[1], (every_t, head_z), 3, bring)

    for copy in remotes[first_remotes:link_remotes]:
        copy.wait_recv()

    for mu in (1, 2, 3):
        third(utp, mu)
        third(utm, mu)
    for mu in (0, 2, 3):
        third(uzp, mu)
        third(uzm, mu)
    moved_rows(utp, 1, (edge_t, head_z), 0, (edge_t, tail_z))
    moved_rows(uzm, 1, (tail_t, zero), 0, (head_t, zero))
    moved_rows(utm, 0, (zero, tail_z), 1, (zero, head_z))
    moved_rows(uzp, 0, (head_t, edge_z), 1, (tail_t, edge_z))
    for k in range(2):
        third(edges, k)
    for k in range(4):
        third(far, k)
    for mu in (0, 1, 3):
        here = gauge(ul, mu)
        put(urp, mu, both(r_ahead, here, gauge(urf, mu)))
        put(urm, mu, both(r_behind, here, gauge(urb, mu)))
    put(edges, 2, both(r_behind, gauge(utp, 2), gauge(far, 0)))
    put(edges, 3, both(r_ahead, gauge(utm, 0), gauge(far, 1)))
    put(edges, 4, both(r_behind, gauge(uzp, 2), gauge(far, 2)))
    put(edges, 5, both(r_ahead, gauge(uzm, 1), gauge(far, 3)))
    put(edges, 6, y_down(gauge(utp, 3)))
    put(edges, 7, y_up(gauge(utm, 0)))
    put(edges, 8, y_down(gauge(uzp, 3)))
    put(edges, 9, y_up(gauge(uzm, 1)))
    put(edges, 10, y_down(gauge(urp, 3)))
    put(edges, 11, y_up(gauge(urm, 2)))

    slot_of = {(0, 1): 0, (1, 0): 1, (0, 2): 2, (2, 0): 3, (1, 2): 4, (2, 1): 5,
               (0, 3): 6, (3, 0): 7, (1, 3): 8, (3, 1): 9, (2, 3): 10, (3, 2): 11}
    plus = (utp, uzp, urp, uyp)
    minus = (utm, uzm, urm, uym)

    def paired(one, two):
        return both(lambda p, q: jnp.concatenate([p, q], 2), one, two)

    def swapped(value):
        return both(lambda v: jnp.concatenate([v[:, :, rows:], v[:, :, :rows]], 2), value)

    planes = [(mu, nu) for mu in range(4) for nu in range(mu + 1, 4)]
    for k, (mu, nu) in enumerate(planes):
        here = paired(gauge(ul, mu), gauge(ul, nu))
        ahead = paired(gauge(plus[mu], nu), gauge(plus[nu], mu))
        walk = product(here, ahead)
        upper = product(walk, swapped(walk), right_dagger=True)
        corner = paired(gauge(edges, slot_of[mu, nu]), gauge(edges, slot_of[nu, mu]))
        side = paired(gauge(minus[nu], mu), gauge(minus[mu], nu))
        back = paired(gauge(minus[nu], nu), gauge(minus[mu], mu))
        lower = product(
            product(here, corner, right_dagger=True), product(side, back, left_dagger=True)
        )
        fs[k] = nine(added(upper, lower, 1), PLAQUETTE)

    for copy in locals_[staged:]:
        copy.wait()
    for copy in remotes[link_remotes:]:
        copy.wait_recv()

    x = spinor(xs)
    y = spinor(ys)
    for mu in range(4):
        if mu == 3:
            ahead = y_up(half(y, 3, 1))
        elif mu == 2:
            ahead = both(r_ahead, gauge(hy, 2), gauge(hyn, 2))
        else:
            ahead = gauge(hyn, mu)
            if mu == 0:
                ahead = signed(ahead, ahead_sign)
        moved = colour(doubled(ul, mu), ahead)
        term = added(outer(gauge(ws, mu), half(y, mu, -1)), outer(moved, half(x, mu, 1)), 1)
        gs[mu] = nine(term, HOPPING)
        parts = gs[mu, :, pl.ds(0, rows)]
        for n in range(1, solves):
            parts = parts + gs[mu, :, pl.ds(n * rows, rows)]
        for k, plane in enumerate(planes):
            if mu in plane:
                parts = parts + fs[k, :, pl.ds(plane.index(mu) * rows, rows)]
        force[mu] = parts

    for copy in remotes:
        copy.wait_send()


def on_device(sizes, links, solutions):
    whole = links.shape
    lanes = whole[-1]
    block = whole[4:6]
    rows = block[0] * block[1]
    links = links.reshape(*whole[:4], rows, lanes)
    n, c, s, a = solutions.shape[:4]
    solutions = solutions.reshape(n, c, s, a, rows, lanes)

    def vmem(*shape):
        return pltpu.VMEM(shape, jnp.float32)

    u = vmem(*links.shape)
    x = vmem(c, s, a, n * rows, lanes)
    unused = vmem(8, lanes) if sizes[2] == 2 else None
    small = links.shape[1:]
    h = vmem(3, c, 2, a, n * rows, lanes)
    h4 = vmem(4, c, 2, a, n * rows, lanes)
    out = pl.pallas_call(
        functools.partial(kernel, sizes, block),
        out_shape=jax.ShapeDtypeStruct((whole[0], 9, rows, lanes), jnp.float32),
        in_specs=[pl.BlockSpec(memory_space=pl.ANY)] * 2,
        out_specs=pl.BlockSpec(memory_space=pltpu.VMEM),
        scratch_shapes=[u] * 6 + [unused or u] + [u] * 4 + [vmem(12, *small), vmem(4, *small)]
        + [x, h4, h4, x, unused or x, x, h, h]
        + [vmem(4, c, 2, a, n * rows, lanes), vmem(6, 9, 2 * rows, lanes),
           vmem(4, 9, n * rows, lanes)]
        + [pltpu.SemaphoreType.DMA((LOCAL_COPIES,)), pltpu.SemaphoreType.DMA((REMOTE_COPIES,)),
           pltpu.SemaphoreType.DMA((REMOTE_COPIES,))],
        compiler_params=pltpu.CompilerParams(collective_id=0, has_side_effects=True),
    )(links, solutions)
    out = pl.pallas_call(
        assembled,
        out_shape=jax.ShapeDtypeStruct(links.shape, jnp.float32),
        in_specs=[pl.BlockSpec(memory_space=pltpu.VMEM)],
        out_specs=pl.BlockSpec(memory_space=pltpu.VMEM),
        compiler_params=pltpu.CompilerParams(vmem_limit_bytes=8 * 2**20),
    )(out)
    return out.reshape(whole)


def assembled(nines, force):
    for mu in range(nines.shape[0]):
        parts = nines[mu]
        mean = (parts[6] + parts[7] + parts[8]) / 3.0
        for k, (i, j) in enumerate(((0, 1), (0, 2), (1, 2))):
            force[mu, 0, i, j] = parts[k]
            force[mu, 0, j, i] = -parts[k]
            force[mu, 1, i, j] = parts[3 + k]
            force[mu, 1, j, i] = parts[3 + k]
        for i in range(3):
            force[mu, 0, i, i] = jnp.zeros_like(mean)
            force[mu, 1, i, i] = parts[6 + i] - mean


def solution(mesh):
    sizes = tuple(mesh.shape[axis] for axis in AXES)
    spec = P(None, None, None, None, *AXES)
    return jax.shard_map(
        functools.partial(on_device, sizes), mesh=mesh, in_specs=(spec, spec), out_specs=spec,
        check_vma=False,
    )
```
